32 devices in a mesh: blk: 8 (over y, x, core), uly: 4 (over z).
Axes of the slice: x: 2, y: 2, z: 4, core: 2. Of those that a mesh axis runs over, the one named last changes fastest.
Arguments:
- queries: bfloat16 [4096, 4096], P(('blk', 'uly')), may hold values from -128 to 128
- keys: bfloat16 [4096, 1024], P(('blk', 'uly')), may hold values from -7 to 7
- values: bfloat16 [4096, 1024], P(('blk', 'uly')), may hold values from -6 to 6
- doc_ids: int32 [4096], P(('blk', 'uly')), may hold values from 0 to 31, never falling along the last dimension, each value on 1 to 512 neighbouring positions
- out_weight: bfloat16 [4096, 4096], P('uly'), may hold values from -0.09375 to 0.09375
Outputs:
- mixed: bfloat16 [4096, 4096], P(('blk', 'uly'))
The draws below stay inside these ranges and needn't reach their ends.
Inputs may be any that keep to these rules, and one draw needn't show every extreme that they name: `doc_ids`: document numbers never fall along the pack; each document holds 1 to 512 consecutive tokens, and some document holds exactly 512.
All inputs are finite; a program needn't handle non-finite values.
Results may differ from the reference program's by a relative error of at most 0.017.
Values may be sent and summed in bfloat16 or wider, within the bound.
A program may use at most 64 MiB of HBM per device.

```python
import math
import jax
import jax.numpy as jnp
import numpy as np
from jax import lax

HEADS = 32
KV_HEADS = 8
HEAD_DIM = 128
OUT_COLS = 4096
Q_WIDTH = 4096
TOKENS = 4096
DOC_MOST = 512
DOCS = 32
N_ULY = 4


def paired_draw(key):
    base = jax.random.fold_in(key, 4242)
    first, second = jax.random.split(base, 2)
    key_rows = jax.random.truncated_normal(first, -6.0, 6.0, (TOKENS, KV_HEADS * HEAD_DIM), jnp.float32)
    query_rows = jax.random.truncated_normal(second, -6.0, 6.0, (TOKENS, HEADS * HEAD_DIM), jnp.float32)
    return (query_rows, key_rows)


def draw_queries(key, part):
    return paired_draw(key)[0].astype(jnp.bfloat16)


def draw_keys(key, part):
    return paired_draw(key)[1].astype(jnp.bfloat16)


def steps_of(key, extent, cuts, least, largest):
    factor_of, own = 1.0, jax.random.fold_in(key, 6)
    for dim, shards_of in cuts:
        steps = jnp.exp(jax.random.uniform(jax.random.fold_in(own, dim), (shards_of,), jnp.float32, least / len(cuts), largest / len(cuts)))
        factor_of = factor_of * jnp.repeat(steps, extent[dim] // shards_of).reshape([-1 if axis == dim else 1 for axis in range(len(extent))])
    return factor_of


def length_profile(amount, total, bound, slope):
    weights = [(1 << 20) // math.isqrt(grade ** slope) + 1 for grade in range(2, amount + 1)]
    rest, given = total - bound - (amount - 1), [1] * (amount - 1)
    while rest > 0:
        movable = [i for i in range(amount - 1) if given[i] < bound]
        pool, budget = sum([weights[i] for i in movable]), rest
        for i in movable:
            extra = min(bound - given[i], max(1, budget * weights[i] // pool), rest)
            given[i] = given[i] + extra
            rest = rest - extra
    return np.array([bound] + given)


def uneven_parts(rng, number_of, total, bound, slope):
    if number_of == 2:
        one = jax.random.randint(rng, (), max(1, total - bound), min(bound, total - 1) + 1)
        return jnp.stack([one, total - one])
    tallies = jnp.asarray(length_profile(number_of, total, bound, slope), jnp.int32)
    twos = (number_of - 1) // 2
    giver, receiver = tallies[1:1 + 2 * twos:2], tallies[2:2 + 2 * twos:2]
    margin = jnp.minimum(giver - 1, bound - receiver)
    passed = jax.random.randint(jax.random.fold_in(rng, 1), (twos,), 0, 1 << 20) % (margin + 1)
    tallies = tallies.at[1:1 + 2 * twos:2].set(giver - passed).at[2:2 + 2 * twos:2].set(receiver + passed)
    return tallies[jax.random.permutation(jax.random.fold_in(rng, 2), number_of)]


def normal_values(rng, shape, scale, most, cuts=(), held_as=jnp.bfloat16):
    gain = steps_of(rng, shape, cuts, -0.22, 0.18) if cuts else 1.0
    values = jax.random.normal(rng, shape, jnp.float32) * scale * gain
    return jnp.minimum(jnp.maximum(values, -most), most).astype(held_as)


def setup_inputs(seed: int = 0) -> dict:
    splits = jax.random.split(jax.random.key(seed), 6)
    return {
        "queries": draw_queries(jax.random.fold_in(splits[5], 71), 0),
        "keys": draw_keys(jax.random.fold_in(splits[5], 71), 0),
        "values": normal_values(splits[2], (TOKENS, KV_HEADS * HEAD_DIM), 1.0, 6.0, ((0, 32),)),
        "doc_ids": jnp.searchsorted(jnp.cumsum(uneven_parts(splits[3], DOCS, TOKENS, DOC_MOST, 1)), jnp.arange(TOKENS), side="right").astype(jnp.int32),
        "out_weight": normal_values(splits[4], (Q_WIDTH, OUT_COLS), Q_WIDTH ** -0.5, 0.09375, ((0, 4),)),
    }


def attend_block(query_block, key_block, value_block, allowed, scale):
    scores = jnp.einsum("qgd,pd->gqp", query_block.astype(jnp.float32), key_block.astype(jnp.float32)) * scale
    scores = jnp.where(allowed[None], scores, -1e30)
    peak = jnp.max(scores, axis=-1, keepdims=True)
    expo = jnp.where(allowed[None], jnp.exp(scores - peak), 0.0)
    total = jnp.sum(expo, axis=-1)
    rounded = expo.astype(jnp.bfloat16).astype(jnp.float32)
    summed = jnp.einsum("gqp,pd->gqd", rounded, value_block.astype(jnp.float32))
    return (summed / total[..., None]).astype(jnp.bfloat16)


def reference(queries, keys, values, doc_ids, out_weight):
    qrows = min(TOKENS, 1024)
    group = HEADS // KV_HEADS
    scale = 1.0 / (HEAD_DIM ** 0.5)
    pieces = []
    for qstart in range(0, TOKENS, qrows):
        kstart = max(0, qstart - DOC_MOST)
        kend = qstart + qrows
        length = kend - kstart
        qpos = qstart + jnp.arange(qrows, dtype=jnp.int32)
        kpos = kstart + jnp.arange(length, dtype=jnp.int32)
        allowed = (kpos[None, :] <= qpos[:, None]) & (doc_ids[kstart:kend][None, :] == doc_ids[qstart:kend][:, None])
        query_block = queries[qstart:kend].reshape(qrows, KV_HEADS, group, HEAD_DIM).transpose(1, 0, 2, 3)
        key_block = keys[kstart:kend].reshape(length, KV_HEADS, HEAD_DIM).transpose(1, 0, 2)
        value_block = values[kstart:kend].reshape(length, KV_HEADS, HEAD_DIM).transpose(1, 0, 2)
        result = lax.map(lambda item: attend_block(item[0], item[1], item[2], allowed, scale), (query_block, key_block, value_block))
        pieces.append(result.transpose(2, 0, 1, 3).reshape(qrows, HEADS * HEAD_DIM))
    attn = jnp.concatenate(pieces, axis=0)
    share = (HEADS // N_ULY) * HEAD_DIM
    mixed = jnp.zeros((TOKENS, OUT_COLS), jnp.float32)
    for group_index in range(N_ULY):
        partial_value = jnp.dot(attn[:, group_index * share:(group_index + 1) * share], out_weight[group_index * share:(group_index + 1) * share], preferred_element_type=jnp.float32)
        partial_value = lax.optimization_barrier(partial_value.astype(jnp.bfloat16))
        mixed = mixed + partial_value.astype(jnp.float32)
    return mixed.astype(jnp.bfloat16)
```

```python
import functools
import math

import jax
import jax.numpy as jnp
from jax import lax
from jax.experimental import pallas as pl
from jax.experimental.pallas import tpu as pltpu
from jax.sharding import PartitionSpec as P

HEAD_DIM = 128
MESH = pl.DeviceIdType.MESH
PIECES = 8


def kernel(n, n_blk, heads, kv_heads, q_ref, k_ref, v_ref, id_ref, w_ref, o_ref,
           qbuf, kbuf, vbuf, idbuf, wbuf, attn, run,
           send_sem, recv_sem, halo_send, halo_recv, run_send, run_recv, w_sem):
    me = lax.axis_index("uly")
    blk = lax.axis_index("blk")
    hd = HEAD_DIM
    rows = q_ref.shape[0]
    block = rows * n
    local_heads = heads // n
    kv_local = max(n, kv_heads) // n
    grouped = local_heads // kv_local
    q_width = local_heads * hd
    kv_width = kv_local * hd
    piece_cols = w_ref.shape[1] // PIECES
    scale = 1.0 / math.sqrt(hd)
    window = n + 1

    def q_cols(dev):
        return pl.ds(pl.multiple_of(dev * q_width, 128), q_width)

    def kv_cols(dev):
        return pl.ds(pl.multiple_of((dev * kv_heads) // n * hd, 128), kv_width)

    w_copy = pltpu.make_async_copy(w_ref, wbuf, w_sem)
    w_copy.start()

    barrier = pltpu.get_barrier_semaphore()
    for off in range(1, n):
        peer = lax.rem(me + off, n)
        pl.semaphore_signal(barrier, inc=1, device_id={"uly": peer}, device_id_type=MESH)

    @pl.when(blk > 0)
    def _():
        pl.semaphore_signal(barrier, inc=1, device_id={"blk": blk - 1}, device_id_type=MESH)

    @pl.when(blk < n_blk - 1)
    def _():
        pl.semaphore_signal(barrier, inc=1, device_id={"blk": blk + 1}, device_id_type=MESH)

    def own_copies():
        return (
            pltpu.make_async_copy(k_ref.at[:, kv_cols(me)], kbuf.at[n + me], recv_sem.at[0, me]),
            pltpu.make_async_copy(v_ref.at[:, kv_cols(me)], vbuf.at[n + me], recv_sem.at[1, me]),
            pltpu.make_async_copy(id_ref, idbuf.at[n + me], recv_sem.at[2, me]),
            pltpu.make_async_copy(q_ref.at[:, q_cols(me)], qbuf.at[me], recv_sem.at[3, me]),
        )

    for copy in own_copies():
        copy.start()

    @pl.when(blk == 0)
    def _():
        kbuf[0:n] = jnp.zeros((n, rows, kv_width), kbuf.dtype)
        vbuf[0:n] = jnp.zeros((n, rows, kv_width), vbuf.dtype)
        idbuf[0:n] = jnp.full((n, 1, rows), -1, jnp.int32)

    pl.semaphore_wait(barrier, n - 1 + jnp.where(blk > 0, 1, 0) + jnp.where(blk < n_blk - 1, 1, 0))

    def remote(src, dst, kind, dev):
        return pltpu.make_async_remote_copy(
            src_ref=src, dst_ref=dst, send_sem=send_sem.at[kind, dev], recv_sem=recv_sem.at[kind, me],
            device_id={"uly": dev}, device_id_type=MESH)

    def kv_sends(dev):
        return (
            remote(id_ref, idbuf.at[n + me], 2, dev),
            remote(k_ref.at[:, kv_cols(dev)], kbuf.at[n + me], 0, dev),
            remote(v_ref.at[:, kv_cols(dev)], vbuf.at[n + me], 1, dev),
        )

    def q_send(dev):
        return remote(q_ref.at[:, q_cols(dev)], qbuf.at[me], 3, dev)

    def each_peer(run_on):
        for off in range(n - 1, 0, -1):
            for dev in (me + off, me - off):
                pl.when((dev >= 0) & (dev < n))(functools.partial(run_on, dev))

    def start_kv(dev):
        for copy in kv_sends(dev):
            copy.start()

    each_peer(start_kv)
    each_peer(lambda dev: q_send(dev).start())

    def halo(slot):
        def one(kind, buf):
            return pltpu.make_async_remote_copy(
                src_ref=buf.at[n + slot], dst_ref=buf.at[slot],
                send_sem=halo_send.at[kind, slot], recv_sem=halo_recv.at[kind, slot],
                device_id={"blk": blk + 1}, device_id_type=MESH)
        return (one(0, kbuf), one(1, vbuf), one(2, idbuf))

    def arrive(slot):
        for kind, buf in ((2, idbuf), (0, kbuf), (1, vbuf)):
            pltpu.make_async_copy(buf.at[n + slot], buf.at[n + slot], recv_sem.at[kind, slot]).wait()

        @pl.when(blk < n_blk - 1)
        def _():
            for copy in halo(slot):
                copy.start()

    arrive(me)
    for off in range(1, n):
        for dev in (me + off, me - off):
            pl.when((dev >= 0) & (dev < n))(functools.partial(arrive, dev))

    @pl.when(blk > 0)
    def _():
        for slot in range(n):
            for copy in halo(slot):
                copy.wait_recv()

    w_copy.wait()

    def attend(d):
        pltpu.make_async_copy(qbuf.at[d], qbuf.at[d], recv_sem.at[3, d]).wait()
        key_ids = jnp.concatenate([idbuf[d + i] for i in range(window)], axis=1)
        query_ids = jnp.broadcast_to(idbuf[n + d], (rows, rows)).T[:, :1]
        col = lax.broadcasted_iota(jnp.int32, (rows, window * rows), 1)
        row = lax.broadcasted_iota(jnp.int32, (rows, window * rows), 0)
        allowed = (key_ids == query_ids) & (col <= row + block)
        for g in range(kv_local):
            key = kbuf[pl.ds(d, window), :, g * hd:(g + 1) * hd].reshape(window * rows, hd)
            value = vbuf[pl.ds(d, window), :, g * hd:(g + 1) * hd].reshape(window * rows, hd)
            for r in range(grouped):
                h = g * grouped + r
                query = qbuf[d, :, h * hd:(h + 1) * hd]
                scores = lax.dot_general(query, key, (((1,), (1,)), ((), ())),
                                         preferred_element_type=jnp.float32) * scale
                scores = jnp.where(allowed, scores, -1e30)
                peak = jnp.max(scores, axis=-1, keepdims=True)
                expo = jnp.exp(scores - peak)
                total = jnp.sum(expo, axis=-1, keepdims=True)
                summed = jnp.dot(expo.astype(jnp.bfloat16), value, preferred_element_type=jnp.float32)
                attn[d, :, h * hd:(h + 1) * hd] = (summed / total).astype(jnp.bfloat16)

    def part(d, p):
        cols = pl.ds(pl.multiple_of(p * piece_cols, 128), piece_cols)
        return jnp.dot(attn[d], wbuf[:, cols], preferred_element_type=jnp.float32)

    def hop(way, d, p, dev):
        return pltpu.make_async_remote_copy(
            src_ref=run.at[way, d, p], dst_ref=run.at[way, d, p],
            send_sem=run_send.at[way, d, p], recv_sem=run_recv.at[way, d, p],
            device_id={"uly": dev}, device_id_type=MESH)

    def landed(way, d, p):
        pltpu.make_async_copy(run.at[way, d, p], run.at[way, d, p], run_recv.at[way, d, p]).wait()

    def pass_on(d, p):
        way = jnp.where(d > me, 0, 1)
        dev = jnp.where(d > me, me + 1, me - 1)
        first = jnp.where(d > me, me, n - 1 - me) == 0
        acc = part(d, p)

        @pl.when(first)
        def _():
            run[way, d, p] = acc.astype(jnp.bfloat16)

        @pl.when(jnp.logical_not(first))
        def _():
            landed(way, d, p)
            run[way, d, p] = (acc + run[way, d, p].astype(jnp.float32)).astype(jnp.bfloat16)

        hop(way, d, p, dev).start()

    def pair(t, carry):
        far, near = n - 1 - t, t
        attend(far)
        attend(near)

        def step(p, inner):
            pl.when(far != me)(functools.partial(pass_on, far, p))
            pl.when(near != me)(functools.partial(pass_on, near, p))
            return inner

        return lax.fori_loop(0, PIECES, step, carry)

    lax.fori_loop(0, n // 2, pair, 0)

    def finish(p, carry):
        cols = pl.ds(pl.multiple_of(p * piece_cols, 128), piece_cols)
        run_sum = part(me, p)
        wbufless = run_sum

        @pl.when(me == 0)
        def _():
            landed(1, me, p)
            o_ref[:, cols] = (wbufless + run[1, me, p].astype(jnp.float32)).astype(o_ref.dtype)

        @pl.when(me == n - 1)
        def _():
            landed(0, me, p)
            o_ref[:, cols] = (wbufless + run[0, me, p].astype(jnp.float32)).astype(o_ref.dtype)

        @pl.when((me > 0) & (me < n - 1))
        def _():
            landed(0, me, p)
            landed(1, me, p)
            both = run[0, me, p].astype(jnp.float32) + run[1, me, p].astype(jnp.float32)
            o_ref[:, cols] = (wbufless + both).astype(o_ref.dtype)

        return carry

    lax.fori_loop(0, PIECES, finish, 0)

    def end_peer(dev):
        for copy in kv_sends(dev):
            copy.wait_send()
        q_send(dev).wait_send()

    each_peer(end_peer)

    @pl.when(blk < n_blk - 1)
    def _():
        for slot in range(n):
            for copy in halo(slot):
                copy.wait_send()

    def end_run(i, carry):
        d, p = i // PIECES, lax.rem(i, PIECES)

        @pl.when(d != me)
        def _():
            hop(jnp.where(d > me, 0, 1), d, p, jnp.where(d > me, me + 1, me - 1)).wait_send()

        return carry

    lax.fori_loop(0, n * PIECES, end_run, 0)


def body(queries, keys, values, doc_ids, out_weight):
    n = lax.axis_size("uly")
    n_blk = lax.axis_size("blk")
    rows = queries.shape[0]
    hd = HEAD_DIM
    heads = queries.shape[1] // hd
    kv_heads = keys.shape[1] // hd
    kv_width = max(n, kv_heads) // n * hd
    q_width = heads // n * hd
    out_cols = out_weight.shape[1]
    vmem = pl.BlockSpec(memory_space=pltpu.VMEM)
    return pl.pallas_call(
        functools.partial(kernel, n, n_blk, heads, kv_heads),
        out_shape=jax.ShapeDtypeStruct((rows, out_cols), jnp.bfloat16),
        in_specs=[vmem] * 4 + [pl.BlockSpec(memory_space=pl.ANY)],
        out_specs=vmem,
        scratch_shapes=[
            pltpu.VMEM((n, rows, q_width), jnp.bfloat16),
            pltpu.VMEM((2 * n, rows, kv_width), jnp.bfloat16),
            pltpu.VMEM((2 * n, rows, kv_width), jnp.bfloat16),
            pltpu.VMEM((2 * n, 1, rows), jnp.int32),
            pltpu.VMEM(out_weight.shape, jnp.bfloat16),
            pltpu.VMEM((n, rows, q_width), jnp.bfloat16),
            pltpu.VMEM((2, n, PIECES, rows, out_cols // PIECES), jnp.bfloat16),
            pltpu.SemaphoreType.DMA((4, n)),
            pltpu.SemaphoreType.DMA((4, n)),
            pltpu.SemaphoreType.DMA((3, n)),
            pltpu.SemaphoreType.DMA((3, n)),
            pltpu.SemaphoreType.DMA((2, n, PIECES)),
            pltpu.SemaphoreType.DMA((2, n, PIECES)),
            pltpu.SemaphoreType.DMA,
        ],
        compiler_params=pltpu.CompilerParams(
            collective_id=0, has_side_effects=True, vmem_limit_bytes=60 * 1024 * 1024
        ),
    )(queries, keys, values, doc_ids.reshape(1, rows), out_weight)


def solution(mesh):
    placed = (
        P(("blk", "uly"), None),
        P(("blk", "uly"), None),
        P(("blk", "uly"), None),
        P(("blk", "uly")),
        P("uly", None),
    )
    return jax.shard_map(
        body, mesh=mesh, in_specs=placed, out_specs=P(("blk", "uly"), None), check_vma=False
    )
```

```python
import functools
import math

import jax
import jax.numpy as jnp
from jax import lax
from jax.experimental import pallas as pl
from jax.experimental.pallas import tpu as pltpu
from jax.sharding import PartitionSpec as P

HEAD_DIM = 128
MESH = pl.DeviceIdType.MESH
PIECES = 8


def kernel(n, n_blk, heads, kv_heads, q_ref, k_ref, v_ref, id_ref, w_ref, o_ref,
           qbuf, kbuf, vbuf, idbuf, wbuf, attn, run,
           send_sem, recv_sem, halo_send, halo_recv, run_send, run_recv, w_sem):
    me = lax.axis_index("uly")
    blk = lax.axis_index("blk")
    hd = HEAD_DIM
    rows = q_ref.shape[0]
    block = rows * n
    local_heads = heads // n
    kv_local = max(n, kv_heads) // n
    grouped = local_heads // kv_local
    q_width = local_heads * hd
    kv_width = kv_local * hd
    piece_cols = w_ref.shape[1] // PIECES
    scale = 1.0 / math.sqrt(hd)
    window = n + 1

    def q_cols(dev):
        return pl.ds(pl.multiple_of(dev * q_width, 128), q_width)

    def kv_cols(dev):
        return pl.ds(pl.multiple_of((dev * kv_heads) // n * hd, 128), kv_width)

    w_copy = pltpu.make_async_copy(w_ref, wbuf, w_sem)
    w_copy.start()

    barrier = pltpu.get_barrier_semaphore()
    for off in range(1, n):
        peer = lax.rem(me + off, n)
        pl.semaphore_signal(barrier, inc=1, device_id={"uly": peer}, device_id_type=MESH)

    @pl.when(blk > 0)
    def _():
        pl.semaphore_signal(barrier, inc=1, device_id={"blk": blk - 1}, device_id_type=MESH)

    @pl.when(blk < n_blk - 1)
    def _():
        pl.semaphore_signal(barrier, inc=1, device_id={"blk": blk + 1}, device_id_type=MESH)

    def own_copies():
        return (
            pltpu.make_async_copy(k_ref.at[:, kv_cols(me)], kbuf.at[n + me], recv_sem.at[0, me]),
            pltpu.make_async_copy(v_ref.at[:, kv_cols(me)], vbuf.at[n + me], recv_sem.at[1, me]),
            pltpu.make_async_copy(id_ref, idbuf.at[n + me], recv_sem.at[2, me]),
            pltpu.make_async_copy(q_ref.at[:, q_cols(me)], qbuf.at[me], recv_sem.at[3, me]),
        )

    for copy in own_copies():
        copy.start()

    @pl.when(blk == 0)
    def _():
        kbuf[0:n] = jnp.zeros((n, rows, kv_width), kbuf.dtype)
        vbuf[0:n] = jnp.zeros((n, rows, kv_width), vbuf.dtype)
        idbuf[0:n] = jnp.full((n, 1, rows), -1, jnp.int32)

    pl.semaphore_wait(barrier, n - 1 + jnp.where(blk > 0, 1, 0) + jnp.where(blk < n_blk - 1, 1, 0))

    def remote(src, dst, kind, dev):
        return pltpu.make_async_remote_copy(
            src_ref=src, dst_ref=dst, send_sem=send_sem.at[kind, dev], recv_sem=recv_sem.at[kind, me],
            device_id={"uly": dev}, device_id_type=MESH)

    def kv_sends(dev):
        return (
            remote(id_ref, idbuf.at[n + me], 2, dev),
            remote(k_ref.at[:, kv_cols(dev)], kbuf.at[n + me], 0, dev),
            remote(v_ref.at[:, kv_cols(dev)], vbuf.at[n + me], 1, dev),
        )

    def q_send(dev):
        return remote(q_ref.at[:, q_cols(dev)], qbuf.at[me], 3, dev)

    def each_peer(run_on):
        for off in range(n - 1, 0, -1):
            for dev in (me + off, me - off):
                pl.when((dev >= 0) & (dev < n))(functools.partial(run_on, dev))

    def start_kv(dev):
        for copy in kv_sends(dev):
            copy.start()

    each_peer(start_kv)
    for i in range(n):
        place = n - 1 - i // 2 if i % 2 == 0 else i // 2
        dev = jnp.where(me < n // 2, place, n - 1 - place)
        pl.when(dev != me)(lambda dev=dev: q_send(dev).start())

    def halo(slot):
        def one(kind, buf):
            return pltpu.make_async_remote_copy(
                src_ref=buf.at[n + slot], dst_ref=buf.at[slot],
                send_sem=halo_send.at[kind, slot], recv_sem=halo_recv.at[kind, slot],
                device_id={"blk": blk + 1}, device_id_type=MESH)
        return (one(0, kbuf), one(1, vbuf), one(2, idbuf))

    def arrive(slot):
        for kind, buf in ((2, idbuf), (0, kbuf), (1, vbuf)):
            pltpu.make_async_copy(buf.at[n + slot], buf.at[n + slot], recv_sem.at[kind, slot]).wait()

        @pl.when(blk < n_blk - 1)
        def _():
            for copy in halo(slot):
                copy.start()

    arrive(me)
    for off in range(1, n):
        for dev in (me + off, me - off):
            pl.when((dev >= 0) & (dev < n))(functools.partial(arrive, dev))

    @pl.when(blk > 0)
    def _():
        for slot in range(n):
            for copy in halo(slot):
                copy.wait_recv()

    w_copy.wait()

    def attend(d):
        pltpu.make_async_copy(qbuf.at[d], qbuf.at[d], recv_sem.at[3, d]).wait()
        key_ids = jnp.concatenate([idbuf[d + i] for i in range(window)], axis=1)
        query_ids = jnp.broadcast_to(idbuf[n + d], (rows, rows)).T[:, :1]
        col = lax.broadcasted_iota(jnp.int32, (rows, window * rows), 1)
        row = lax.broadcasted_iota(jnp.int32, (rows, window * rows), 0)
        allowed = (key_ids == query_ids) & (col <= row + block)
        for g in range(kv_local):
            key = kbuf[pl.ds(d, window), :, g * hd:(g + 1) * hd].reshape(window * rows, hd)
            value = vbuf[pl.ds(d, window), :, g * hd:(g + 1) * hd].reshape(window * rows, hd)
            for r in range(grouped):
                h = g * grouped + r
                query = qbuf[d, :, h * hd:(h + 1) * hd]
                scores = lax.dot_general(query, key, (((1,), (1,)), ((), ())),
                                         preferred_element_type=jnp.float32) * scale
                scores = jnp.where(allowed, scores, -1e30)
                peak = jnp.max(scores, axis=-1, keepdims=True)
                expo = jnp.exp(scores - peak)
                total = jnp.sum(expo, axis=-1, keepdims=True)
                summed = jnp.dot(expo.astype(jnp.bfloat16), value, preferred_element_type=jnp.float32)
                attn[d, :, h * hd:(h + 1) * hd] = (summed / total).astype(jnp.bfloat16)

    def part(d, p):
        cols = pl.ds(pl.multiple_of(p * piece_cols, 128), piece_cols)
        return jnp.dot(attn[d], wbuf[:, cols], preferred_element_type=jnp.float32)

    def hop(way, d, p, dev):
        return pltpu.make_async_remote_copy(
            src_ref=run.at[way, d, p], dst_ref=run.at[way, d, p],
            send_sem=run_send.at[way, d, p], recv_sem=run_recv.at[way, d, p],
            device_id={"uly": dev}, device_id_type=MESH)

    def landed(way, d, p):
        pltpu.make_async_copy(run.at[way, d, p], run.at[way, d, p], run_recv.at[way, d, p]).wait()

    def pass_on(d, p):
        way = jnp.where(d > me, 0, 1)
        dev = jnp.where(d > me, me + 1, me - 1)
        first = jnp.where(d > me, me, n - 1 - me) == 0
        acc = part(d, p)

        @pl.when(first)
        def _():
            run[way, d, p] = acc.astype(jnp.bfloat16)

        @pl.when(jnp.logical_not(first))
        def _():
            landed(way, d, p)
            run[way, d, p] = (acc + run[way, d, p].astype(jnp.float32)).astype(jnp.bfloat16)

        hop(way, d, p, dev).start()

    low = me < n // 2
    end = (me == 0) | (me == n - 1)

    def pair(t, carry):
        one = jnp.where(low, n - 1 - t, t)
        two = n - 1 - one

        def pieces(which):
            def step(p, inner):
                for d in which:
                    pl.when(d != me)(functools.partial(pass_on, d, p))
                return inner
            lax.fori_loop(0, PIECES, step, 0)

        attend(one)
        pl.when(end)(functools.partial(pieces, (one,)))
        attend(two)
        pl.when(end)(functools.partial(pieces, (two,)))
        pl.when(jnp.logical_not(end))(functools.partial(pieces, (one, two)))
        return carry

    lax.fori_loop(0, n // 2, pair, 0)

    def finish(p, carry):
        cols = pl.ds(pl.multiple_of(p * piece_cols, 128), piece_cols)
        own = part(me, p)

        @pl.when(me == 0)
        def _():
            landed(1, me, p)
            o_ref[:, cols] = (own + run[1, me, p].astype(jnp.float32)).astype(o_ref.dtype)

        @pl.when(me == n - 1)
        def _():
            landed(0, me, p)
            o_ref[:, cols] = (own + run[0, me, p].astype(jnp.float32)).astype(o_ref.dtype)

        @pl.when((me > 0) & (me < n - 1))
        def _():
            landed(0, me, p)
            landed(1, me, p)
            both = run[0, me, p].astype(jnp.float32) + run[1, me, p].astype(jnp.float32)
            o_ref[:, cols] = (own + both).astype(o_ref.dtype)

        return carry

    lax.fori_loop(0, PIECES, finish, 0)

    def end_peer(dev):
        for copy in kv_sends(dev):
            copy.wait_send()
        q_send(dev).wait_send()

    each_peer(end_peer)

    @pl.when(blk < n_blk - 1)
    def _():
        for slot in range(n):
            for copy in halo(slot):
                copy.wait_send()

    def end_run(i, carry):
        d, p = i // PIECES, lax.rem(i, PIECES)

        @pl.when(d != me)
        def _():
            hop(jnp.where(d > me, 0, 1), d, p, jnp.where(d > me, me + 1, me - 1)).wait_send()

        return carry

    lax.fori_loop(0, n * PIECES, end_run, 0)


def body(queries, keys, values, doc_ids, out_weight):
    n = lax.axis_size("uly")
    n_blk = lax.axis_size("blk")
    rows = queries.shape[0]
    hd = HEAD_DIM
    heads = queries.shape[1] // hd
    kv_heads = keys.shape[1] // hd
    kv_width = max(n, kv_heads) // n * hd
    q_width = heads // n * hd
    out_cols = out_weight.shape[1]
    vmem = pl.BlockSpec(memory_space=pltpu.VMEM)
    return pl.pallas_call(
        functools.partial(kernel, n, n_blk, heads, kv_heads),
        out_shape=jax.ShapeDtypeStruct((rows, out_cols), jnp.bfloat16),
        in_specs=[vmem] * 4 + [pl.BlockSpec(memory_space=pl.ANY)],
        out_specs=vmem,
        scratch_shapes=[
            pltpu.VMEM((n, rows, q_width), jnp.bfloat16),
            pltpu.VMEM((2 * n, rows, kv_width), jnp.bfloat16),
            pltpu.VMEM((2 * n, rows, kv_width), jnp.bfloat16),
            pltpu.VMEM((2 * n, 1, rows), jnp.int32),
            pltpu.VMEM(out_weight.shape, jnp.bfloat16),
            pltpu.VMEM((n, rows, q_width), jnp.bfloat16),
            pltpu.VMEM((2, n, PIECES, rows, out_cols // PIECES), jnp.bfloat16),
            pltpu.SemaphoreType.DMA((4, n)),
            pltpu.SemaphoreType.DMA((4, n)),
            pltpu.SemaphoreType.DMA((3, n)),
            pltpu.SemaphoreType.DMA((3, n)),
            pltpu.SemaphoreType.DMA((2, n, PIECES)),
            pltpu.SemaphoreType.DMA((2, n, PIECES)),
            pltpu.SemaphoreType.DMA,
        ],
        compiler_params=pltpu.CompilerParams(
            collective_id=0, has_side_effects=True, vmem_limit_bytes=60 * 1024 * 1024
        ),
    )(queries, keys, values, doc_ids.reshape(1, rows), out_weight)


def solution(mesh):
    placed = (
        P(("blk", "uly"), None),
        P(("blk", "uly"), None),
        P(("blk", "uly"), None),
        P(("blk", "uly")),
        P("uly", None),
    )
    return jax.shard_map(
        body, mesh=mesh, in_specs=placed, out_specs=P(("blk", "uly"), None), check_vma=False
    )
```

```python
import functools
import math

import jax
import jax.numpy as jnp
from jax import lax
from jax.experimental import pallas as pl
from jax.experimental.pallas import tpu as pltpu
from jax.sharding import PartitionSpec as P

HEAD_DIM = 128
MESH = pl.DeviceIdType.MESH
PIECES = 4


def kernel(n, n_blk, heads, kv_heads, q_ref, k_ref, v_ref, id_ref, w_ref, o_ref,
           qbuf, kbuf, vbuf, idbuf, wbuf, attn, run,
           send_sem, recv_sem, halo_send, halo_recv, run_send, run_recv, w_sem):
    me = lax.axis_index("uly")
    blk = lax.axis_index("blk")
    hd = HEAD_DIM
    rows = q_ref.shape[0]
    block = rows * n
    local_heads = heads // n
    kv_local = max(n, kv_heads) // n
    grouped = local_heads // kv_local
    q_width = local_heads * hd
    kv_width = kv_local * hd
    piece_cols = w_ref.shape[1] // PIECES
    scale = 1.0 / math.sqrt(hd)
    window = n + 1

    def q_cols(dev):
        return pl.ds(pl.multiple_of(dev * q_width, 128), q_width)

    def kv_cols(dev):
        return pl.ds(pl.multiple_of((dev * kv_heads) // n * hd, 128), kv_width)

    w_copy = pltpu.make_async_copy(w_ref, wbuf, w_sem)
    w_copy.start()

    barrier = pltpu.get_barrier_semaphore()
    for off in range(1, n):
        peer = lax.rem(me + off, n)
        pl.semaphore_signal(barrier, inc=1, device_id={"uly": peer}, device_id_type=MESH)

    @pl.when(blk > 0)
    def _():
        pl.semaphore_signal(barrier, inc=1, device_id={"blk": blk - 1}, device_id_type=MESH)

    @pl.when(blk < n_blk - 1)
    def _():
        pl.semaphore_signal(barrier, inc=1, device_id={"blk": blk + 1}, device_id_type=MESH)

    def own_copies():
        return (
            pltpu.make_async_copy(k_ref.at[:, kv_cols(me)], kbuf.at[n + me], recv_sem.at[0, me]),
            pltpu.make_async_copy(v_ref.at[:, kv_cols(me)], vbuf.at[n + me], recv_sem.at[1, me]),
            pltpu.make_async_copy(id_ref, idbuf.at[n + me], recv_sem.at[2, me]),
            pltpu.make_async_copy(q_ref.at[:, q_cols(me)], qbuf.at[me], recv_sem.at[3, me]),
        )

    for copy in own_copies():
        copy.start()

    @pl.when(blk == 0)
    def _():
        kbuf[0:n] = jnp.zeros((n, rows, kv_width), kbuf.dtype)
        vbuf[0:n] = jnp.zeros((n, rows, kv_width), vbuf.dtype)
        idbuf[0:n] = jnp.full((n, 1, rows), -1, jnp.int32)

    pl.semaphore_wait(barrier, n - 1 + jnp.where(blk > 0, 1, 0) + jnp.where(blk < n_blk - 1, 1, 0))

    def remote(src, dst, kind, dev):
        return pltpu.make_async_remote_copy(
            src_ref=src, dst_ref=dst, send_sem=send_sem.at[kind, dev], recv_sem=recv_sem.at[kind, me],
            device_id={"uly": dev}, device_id_type=MESH)

    def kv_sends(dev):
        return (
            remote(id_ref, idbuf.at[n + me], 2, dev),
            remote(k_ref.at[:, kv_cols(dev)], kbuf.at[n + me], 0, dev),
            remote(v_ref.at[:, kv_cols(dev)], vbuf.at[n + me], 1, dev),
        )

    def q_send(dev):
        return remote(q_ref.at[:, q_cols(dev)], qbuf.at[me], 3, dev)

    def each_peer(run_on):
        for off in range(n - 1, 0, -1):
            for dev in (me + off, me - off):
                pl.when((dev >= 0) & (dev < n))(functools.partial(run_on, dev))

    def start_kv(dev):
        for copy in kv_sends(dev):
            copy.start()

    each_peer(start_kv)
    for i in range(n):
        place = n - 1 - i // 2 if i % 2 == 0 else i // 2
        dev = jnp.where(me < n // 2, place, n - 1 - place)
        pl.when(dev != me)(lambda dev=dev: q_send(dev).start())

    def halo(slot):
        def one(kind, buf):
            return pltpu.make_async_remote_copy(
                src_ref=buf.at[n + slot], dst_ref=buf.at[slot],
                send_sem=halo_send.at[kind, slot], recv_sem=halo_recv.at[kind, slot],
                device_id={"blk": blk + 1}, device_id_type=MESH)
        return (one(0, kbuf), one(1, vbuf), one(2, idbuf))

    def arrive(slot):
        for kind, buf in ((2, idbuf), (0, kbuf), (1, vbuf)):
            pltpu.make_async_copy(buf.at[n + slot], buf.at[n + slot], recv_sem.at[kind, slot]).wait()

        @pl.when(blk < n_blk - 1)
        def _():
            for copy in halo(slot):
                copy.start()

    arrive(me)
    for off in range(1, n):
        for dev in (me + off, me - off):
            pl.when((dev >= 0) & (dev < n))(functools.partial(arrive, dev))

    @pl.when(blk > 0)
    def _():
        for slot in range(n):
            for copy in halo(slot):
                copy.wait_recv()

    w_copy.wait()

    def attend(d):
        pltpu.make_async_copy(qbuf.at[d], qbuf.at[d], recv_sem.at[3, d]).wait()
        key_ids = jnp.concatenate([idbuf[d + i] for i in range(window)], axis=1)
        query_ids = jnp.broadcast_to(idbuf[n + d], (rows, rows)).T[:, :1]
        col = lax.broadcasted_iota(jnp.int32, (rows, window * rows), 1)
        row = lax.broadcasted_iota(jnp.int32, (rows, window * rows), 0)
        allowed = (key_ids == query_ids) & (col <= row + block)
        for g in range(kv_local):
            key = kbuf[pl.ds(d, window), :, g * hd:(g + 1) * hd].reshape(window * rows, hd)
            value = vbuf[pl.ds(d, window), :, g * hd:(g + 1) * hd].reshape(window * rows, hd)
            for r in range(grouped):
                h = g * grouped + r
                query = qbuf[d, :, h * hd:(h + 1) * hd]
                scores = lax.dot_general(query, key, (((1,), (1,)), ((), ())),
                                         preferred_element_type=jnp.float32) * scale
                scores = jnp.where(allowed, scores, -1e30)
                peak = jnp.max(scores, axis=-1, keepdims=True)
                expo = jnp.exp(scores - peak)
                total = jnp.sum(expo, axis=-1, keepdims=True)
                summed = jnp.dot(expo.astype(jnp.bfloat16), value, preferred_element_type=jnp.float32)
                attn[d, :, h * hd:(h + 1) * hd] = (summed / total).astype(jnp.bfloat16)

    def part(d, p):
        cols = pl.ds(pl.multiple_of(p * piece_cols, 128), piece_cols)
        return jnp.dot(attn[d], wbuf[:, cols], preferred_element_type=jnp.float32)

    def hop(way, d, p, dev):
        return pltpu.make_async_remote_copy(
            src_ref=run.at[way, d, p], dst_ref=run.at[way, d, p],
            send_sem=run_send.at[way, d, p], recv_sem=run_recv.at[way, d, p],
            device_id={"uly": dev}, device_id_type=MESH)

    def landed(way, d, p):
        pltpu.make_async_copy(run.at[way, d, p], run.at[way, d, p], run_recv.at[way, d, p]).wait()

    def pass_on(d, p):
        way = jnp.where(d > me, 0, 1)
        dev = jnp.where(d > me, me + 1, me - 1)
        first = jnp.where(d > me, me, n - 1 - me) == 0
        acc = part(d, p)

        @pl.when(first)
        def _():
            run[way, d, p] = acc.astype(jnp.bfloat16)

        @pl.when(jnp.logical_not(first))
        def _():
            landed(way, d, p)
            run[way, d, p] = (acc + run[way, d, p].astype(jnp.float32)).astype(jnp.bfloat16)

        hop(way, d, p, dev).start()

    low = me < n // 2
    end = (me == 0) | (me == n - 1)

    def pair(t, carry):
        one = jnp.where(low, n - 1 - t, t)
        two = n - 1 - one

        def pieces(which):
            def step(p, inner):
                for d in which:
                    pl.when(d != me)(functools.partial(pass_on, d, p))
                return inner
            lax.fori_loop(0, PIECES, step, 0)

        attend(one)
        pl.when(end)(functools.partial(pieces, (one,)))
        attend(two)
        pl.when(end)(functools.partial(pieces, (two,)))
        pl.when(jnp.logical_not(end))(functools.partial(pieces, (one, two)))
        return carry

    lax.fori_loop(0, n // 2, pair, 0)

    def finish(p, carry):
        cols = pl.ds(pl.multiple_of(p * piece_cols, 128), piece_cols)
        own = part(me, p)

        @pl.when(me == 0)
        def _():
            landed(1, me, p)
            o_ref[:, cols] = (own + run[1, me, p].astype(jnp.float32)).astype(o_ref.dtype)

        @pl.when(me == n - 1)
        def _():
            landed(0, me, p)
            o_ref[:, cols] = (own + run[0, me, p].astype(jnp.float32)).astype(o_ref.dtype)

        @pl.when((me > 0) & (me < n - 1))
        def _():
            landed(0, me, p)
            landed(1, me, p)
            both = run[0, me, p].astype(jnp.float32) + run[1, me, p].astype(jnp.float32)
            o_ref[:, cols] = (own + both).astype(o_ref.dtype)

        return carry

    lax.fori_loop(0, PIECES, finish, 0)

    def end_peer(dev):
        for copy in kv_sends(dev):
            copy.wait_send()
        q_send(dev).wait_send()

    each_peer(end_peer)

    @pl.when(blk < n_blk - 1)
    def _():
        for slot in range(n):
            for copy in halo(slot):
                copy.wait_send()

    def end_run(i, carry):
        d, p = i // PIECES, lax.rem(i, PIECES)

        @pl.when(d != me)
        def _():
            hop(jnp.where(d > me, 0, 1), d, p, jnp.where(d > me, me + 1, me - 1)).wait_send()

        return carry

    lax.fori_loop(0, n * PIECES, end_run, 0)


def body(queries, keys, values, doc_ids, out_weight):
    n = lax.axis_size("uly")
    n_blk = lax.axis_size("blk")
    rows = queries.shape[0]
    hd = HEAD_DIM
    heads = queries.shape[1] // hd
    kv_heads = keys.shape[1] // hd
    kv_width = max(n, kv_heads) // n * hd
    q_width = heads // n * hd
    out_cols = out_weight.shape[1]
    vmem = pl.BlockSpec(memory_space=pltpu.VMEM)
    return pl.pallas_call(
        functools.partial(kernel, n, n_blk, heads, kv_heads),
        out_shape=jax.ShapeDtypeStruct((rows, out_cols), jnp.bfloat16),
        in_specs=[vmem] * 4 + [pl.BlockSpec(memory_space=pl.ANY)],
        out_specs=vmem,
        scratch_shapes=[
            pltpu.VMEM((n, rows, q_width), jnp.bfloat16),
            pltpu.VMEM((2 * n, rows, kv_width), jnp.bfloat16),
            pltpu.VMEM((2 * n, rows, kv_width), jnp.bfloat16),
            pltpu.VMEM((2 * n, 1, rows), jnp.int32),
            pltpu.VMEM(out_weight.shape, jnp.bfloat16),
            pltpu.VMEM((n, rows, q_width), jnp.bfloat16),
            pltpu.VMEM((2, n, PIECES, rows, out_cols // PIECES), jnp.bfloat16),
            pltpu.SemaphoreType.DMA((4, n)),
            pltpu.SemaphoreType.DMA((4, n)),
            pltpu.SemaphoreType.DMA((3, n)),
            pltpu.SemaphoreType.DMA((3, n)),
            pltpu.SemaphoreType.DMA((2, n, PIECES)),
            pltpu.SemaphoreType.DMA((2, n, PIECES)),
            pltpu.SemaphoreType.DMA,
        ],
        compiler_params=pltpu.CompilerParams(
            collective_id=0, has_side_effects=True, vmem_limit_bytes=60 * 1024 * 1024
        ),
    )(queries, keys, values, doc_ids.reshape(1, rows), out_weight)


def solution(mesh):
    placed = (
        P(("blk", "uly"), None),
        P(("blk", "uly"), None),
        P(("blk", "uly"), None),
        P(("blk", "uly")),
        P("uly", None),
    )
    return jax.shard_map(
        body, mesh=mesh, in_specs=placed, out_specs=P(("blk", "uly"), None), check_vma=False
    )
```
